32 devices in a mesh: wide: 8 (over z, x), narrow: 4 (over y, core).
Axes of the slice: x: 2, y: 2, z: 4, core: 2. Of those that a mesh axis runs over, the one named last changes fastest.
Arguments:
- activations: bfloat16 [2048, 16384], P('wide', 'narrow'), may hold values from -6 to 6
- grad_out: bfloat16 [2048, 8192], P('narrow', 'wide'), may hold values from -0.125 to 0.125
- momentum: float32 [8192, 16384], P('wide', 'narrow'), may hold values from -90 to 90
- right_factor: float32 [16384, 512], P('narrow'), may hold values from -0.046875 to 0.046875
Outputs:
- new_momentum: float32 [8192, 16384], P('wide', 'narrow')
- new_right: float32 [16384, 512], P('narrow')
- update: bfloat16 [8192, 16384], P('wide', 'narrow')
The draws below stay inside these ranges and needn't reach their ends.
All inputs are finite; a program needn't handle non-finite values.
Results may differ from the reference program's by a relative error of at most 0.0012.
Values may be sent and summed in bfloat16 or wider, within the bound.
No kernel may reach another device: no remote copies, remote signals or barrier semaphores. Data moves between devices by JAX's collectives and lax.ppermute only.
A program may use at most 128 MiB of HBM per device.

```python
import math
import jax
import jax.numpy as jnp
from jax import lax

DOUT = 8192
DIN = 16384
RANK = 512
TOKENS = 2048


def draw_momentum(key, part):
    base = jax.random.fold_in(key, 31)
    first = jax.random.fold_in(base, 0)
    row_scale = 0.5 + jnp.arange(DOUT, dtype=jnp.float32) / (DOUT - 1)
    col_scale = 0.5 + jnp.arange(DIN, dtype=jnp.float32) / (DIN - 1)
    values = jax.random.truncated_normal(first, -4.0, 4.0, (DOUT, DIN), jnp.float32)
    return (values * row_scale[:, None] * col_scale[None, :]).astype(jnp.float32)


def block_scale(stream_key, shape, cuts, least, largest):
    def one(position, shards_of):
        draws = jax.random.uniform(jax.random.fold_in(jax.random.fold_in(stream_key, 6), position), (shards_of,), jnp.float32, least / len(cuts), largest / len(cuts))
        return jnp.repeat(jnp.exp(draws), shape[position] // shards_of).reshape((-1,) + (1,) * (len(shape) - position - 1))

    gain = one(*cuts[0])
    for cut in cuts[1:]:
        gain = gain * one(*cut)
    return gain


def bell_draw(stream_key, extent, spread, bound, shards=(), held_as=jnp.bfloat16):
    drawn = spread * jax.random.normal(stream_key, extent, jnp.float32)
    if shards:
        drawn = drawn * block_scale(stream_key, extent, shards, -0.22, 0.18)
    return jnp.clip(drawn, -bound, bound).astype(held_as)


def setup_inputs(seed: int = 0) -> dict:
    key_list = jax.random.split(jax.random.key(seed), 5)
    return {
        "activations": bell_draw(key_list[0], (TOKENS, DIN), 1.0, 6.0, ((0, 8), (1, 4))),
        "grad_out": bell_draw(key_list[1], (TOKENS, DOUT), TOKENS ** -0.5, 0.125, ((0, 4), (1, 8))),
        "momentum": draw_momentum(jax.random.fold_in(key_list[4], 71), 0),
        "right_factor": bell_draw(key_list[3], (DIN, RANK), DIN ** -0.5, 0.046875, ((0, 4),), jnp.float32),
    }


FEEDBACK = 0.05
EPSILON = 1e-06

def reference(activations, grad_out, momentum, right_factor):
    highest = lax.Precision.HIGHEST
    gradient = lax.dot_general(grad_out.astype(jnp.float32), activations.astype(jnp.float32), (((0,), (0,)), ((), ())), preferred_element_type=jnp.float32)
    buffer = momentum + gradient
    left_factor = jnp.dot(buffer.astype(jnp.float32), right_factor.astype(jnp.float32), precision=highest, preferred_element_type=jnp.float32)
    gram_matrix = jnp.dot(left_factor.T.astype(jnp.float32), left_factor.astype(jnp.float32), precision=highest, preferred_element_type=jnp.float32)
    lower_factor = jnp.linalg.cholesky(gram_matrix)
    ortho_left = jax.scipy.linalg.solve_triangular(lower_factor, left_factor.T, lower=True).T
    right_raw = lax.dot_general(buffer.astype(jnp.float32), ortho_left.astype(jnp.float32), (((0,), (0,)), ((), ())), precision=highest, preferred_element_type=jnp.float32)
    feedback = lax.dot_general(ortho_left.astype(jnp.float32), right_raw.astype(jnp.float32), (((1,), (1,)), ((), ())), precision=highest, preferred_element_type=jnp.float32)
    new_momentum = buffer - FEEDBACK * feedback
    col_squares = lax.optimization_barrier(jnp.sum(right_raw * right_raw, axis=0))
    new_right = right_raw / (jnp.sqrt(col_squares) + EPSILON)
    update_scale = math.sqrt(DOUT * DIN / RANK)
    product = lax.dot_general(ortho_left.astype(jnp.float32), new_right.astype(jnp.float32), (((1,), (1,)), ((), ())), precision=highest, preferred_element_type=jnp.float32)
    update = (update_scale * product).astype(jnp.bfloat16)
    return (new_momentum, new_right, update)
```

```python
import math

import jax
import jax.numpy as jnp
from jax import lax
from jax.experimental import pallas as pl
from jax.experimental.pallas import tpu as pltpu
from jax.sharding import PartitionSpec as P


FEEDBACK = 0.05
EPSILON = 1e-06
LANES = 128
CORES = 2
TILE = 512
PAD = 16
BLOCK = 128
UNROLL = 8

HIGH = lax.Precision.HIGH
HIGHEST = lax.Precision.HIGHEST
F32 = jnp.float32
F16 = jnp.float16
BF16 = jnp.bfloat16


def split(x):
    hi = lax.reduce_precision(x, exponent_bits=8, mantissa_bits=7)
    return hi.astype(BF16), (x - hi).astype(BF16)


def dot(a, b, ca, cb, precision=None):
    return lax.dot_general(
        a, b, (((ca,), (cb,)), ((), ())), precision=precision, preferred_element_type=F32
    )


def put(pieces, starts, shape, axis):
    out = jnp.zeros(shape, pieces[0].dtype)
    for piece, start in zip(pieces, starts):
        out = lax.dynamic_update_slice_in_dim(out, piece, start, axis)
    return out


class Ring:
    def __init__(self, name, outer, inner):
        self.name, self.outer, self.inner = name, outer, inner
        index = lax.axis_index(name)
        self.o, self.i = index // inner, lax.rem(index, inner)

    def send(self, x, do, di):
        o, i = self.outer, self.inner
        if do % o == 0 and di % i == 0:
            return x
        pairs = [
            (a * i + b, ((a + do) % o) * i + (b + di) % i) for a in range(o) for b in range(i)
        ]
        return lax.ppermute(x, self.name, pairs)

    def at(self, do, di):
        o, i = self.outer, self.inner
        return lax.rem(self.o + do % o, o) * i + lax.rem(self.i + di % i, i)

    def order(self):
        return [(s, d) for s in range(self.outer) for d in range(self.inner)]

    def blocks(self, x):
        found = []
        for s, d in self.order():
            found.append(self.send(x, s, d))
        return jnp.concatenate(found, axis=0)

    def gather(self, x, spread=False):
        found, held, aside = {}, x, {}
        for s in range(self.outer):
            held = self.send(held, 1, 0) if s else held
            found[s, 0] = held
            for d in range(1, self.inner):
                if spread and s == self.outer - 1:
                    half = x.shape[1] // 2
                    near = self.send(held[:, :half], 0, d)
                    far = self.send(aside[d][:, half:], 1, 0)
                    found[s, d] = jnp.concatenate([near, far], axis=1)
                else:
                    aside[d] = found[s, d] = self.send(held, 0, d)
        return [found[key] for key in self.order()]

    def scatter_sum(self, piece):
        total = None
        for j in range(self.outer):
            back = -1 - j
            mine = piece(self.at(back, 0))
            for d in range(1, self.inner):
                got = self.send(piece(self.at(back, d)), 0, d)
                mine = mine + got
            if total is not None:
                total = self.send(total, 1, 0)
            total = mine if total is None else total + mine
        return total

    def total(self, x):
        count, step = self.outer * self.inner, 1
        while step < count:
            got = lax.ppermute(x, self.name, [(k, k ^ step) for k in range(count)])
            x = x + got
            step *= 2
        return x


def narrow_sum(ring, x, width):
    cut = lambda index: lax.dynamic_slice_in_dim(x, index * width, width, 1)
    keep = [cut(ring.at(s, 0)) for s in range(ring.outer)]
    give = [cut(ring.at(s, 1)) for s in range(ring.outer)]
    got = ring.send(jnp.concatenate(give, axis=1), 0, 1)
    kept = [k + got[:, s * width : (s + 1) * width] for s, k in enumerate(keep)]
    total = kept[0]
    for s in range(1, ring.outer):
        got = ring.send(kept[s], s, 0)
        total = total + got
    return total


def narrow_collect(ring, x, axis):
    size = x.shape[axis]
    shape = list(x.shape)
    shape[axis] = size * ring.outer * ring.inner
    mine = []
    for s in range(ring.outer):
        mine.append(ring.send(x, s, 0))
    other = ring.send(jnp.concatenate(mine, axis=axis), 0, 1)
    pieces, starts = [], []
    for s in range(ring.outer):
        pieces += [mine[s], lax.slice_in_dim(other, s * size, (s + 1) * size, axis=axis)]
        starts += [ring.at(-s, 0) * size, ring.at(-s, 1) * size]
    return put(pieces, starts, shape, axis)


def buffer_kernel(count, grads, left_hi, left_lo, momentum, *refs):
    acts, (buffer_out, product_out) = refs[:count], refs[-2:]
    rows = jnp.concatenate([a[...] for a in acts], axis=0)
    buffer = momentum[...] + jnp.dot(grads[...], rows, preferred_element_type=F32)
    buffer_out[...] = buffer
    hi = buffer.astype(BF16)
    lo = (buffer - hi.astype(F32)).astype(BF16)
    product = jnp.dot(left_hi[...], hi, preferred_element_type=F32)
    product += jnp.dot(left_hi[...], lo, preferred_element_type=F32)
    product += jnp.dot(left_lo[...], hi, preferred_element_type=F32)
    product_out[...] = product


def buffer_call(half, grads, left_hi, left_lo, momentum, acts, buffer):
    rows, columns = momentum.shape
    rank = left_hi.shape[0]
    width = acts[0].shape[1]
    tile = min(TILE, width)
    first = half * width // tile
    resident = lambda a: pl.BlockSpec(a.shape, lambda j: (0, 0), pipeline_mode=pl.Buffered(1))
    moving = lambda r: pl.BlockSpec((r, tile), lambda j: (0, j))
    placed = pl.BlockSpec((rows, tile), lambda j: (0, first + j))
    in_specs = [resident(grads), resident(left_hi), resident(left_lo), placed]
    in_specs += [moving(a.shape[0]) for a in acts]
    args = [grads, left_hi, left_lo, momentum, *acts]
    aliases = {}
    if buffer is not None:
        aliases = {len(args): 0}
        in_specs.append(pl.BlockSpec(memory_space=pl.ANY))
        args.append(buffer)
    tokens = grads.shape[1]
    flops = 2 * rows * width * (tokens + 3 * rank)
    count = len(acts)
    return pl.pallas_call(
        lambda *refs: buffer_kernel(count, *refs),
        grid=(width // tile,),
        in_specs=in_specs,
        out_specs=[placed, moving(rank)],
        out_shape=[
            jax.ShapeDtypeStruct((rows, columns), F32),
            jax.ShapeDtypeStruct((rank, width), F32),
        ],
        input_output_aliases=aliases,
        compiler_params=pltpu.CompilerParams(
            dimension_semantics=("arbitrary",), vmem_limit_bytes=56 << 20
        ),
        cost_estimate=pl.CostEstimate(
            flops=flops, transcendentals=0, bytes_accessed=width * (8 * rows + 2 * tokens + 4 * rank)
        ),
        name="buffer_product",
    )(*args)


def feedback_kernel(places, ortho, buffer, *refs):
    del places
    rights, (out, squares) = refs[:-2], refs[-2:]
    for k, right in enumerate(rights):

        @pl.when(pl.program_id(0) == k)
        def _(right=right):
            product = dot(ortho[...], right[...].astype(BF16), 1, 1)
            out[...] = buffer[...] - product
            square = jnp.sum(right[...] * right[...], axis=0, keepdims=True)
            squares[...] = square if k == 0 else squares[...] + square


def feedback_call(ortho, buffer, rights, places):
    rows = buffer.shape[0]
    strip, rank = rights[0].shape
    whole = lambda a: pl.BlockSpec(a.shape, lambda k, p: (0, 0), pipeline_mode=pl.Buffered(1))
    placed = pl.BlockSpec((rows, strip), lambda k, p: (0, p[k]))
    count = len(rights)
    return pl.pallas_call(
        feedback_kernel,
        grid_spec=pltpu.PrefetchScalarGridSpec(
            num_scalar_prefetch=1,
            grid=(count,),
            in_specs=[whole(ortho), placed] + [whole(r) for r in rights],
            out_specs=[placed, pl.BlockSpec((1, rank), lambda k, p: (0, 0))],
        ),
        out_shape=[
            jax.ShapeDtypeStruct(buffer.shape, F32),
            jax.ShapeDtypeStruct((1, rank), F32),
        ],
        input_output_aliases={2: 0},
        compiler_params=pltpu.CompilerParams(
            dimension_semantics=("arbitrary",), vmem_limit_bytes=32 << 20
        ),
        cost_estimate=pl.CostEstimate(
            flops=2 * rows * strip * rank * count,
            transcendentals=0,
            bytes_accessed=8 * rows * strip * count,
        ),
        name="feedback",
    )(places, ortho, buffer, *rights)


def update_kernel(q_hi, q_lo, inv_norm, raw, update, right):
    value = raw[...]
    right[...] = value * inv_norm[...]
    hi = value.astype(BF16)
    lo = (value - hi.astype(F32)).astype(BF16)
    product = dot(q_hi[...], hi, 1, 1) + dot(q_hi[...], lo, 1, 1) + dot(q_lo[...], hi, 1, 1)
    update[...] = product.astype(BF16)


def update_call(q_hi, q_lo, inv_norm, raw):
    rows, rank = q_hi.shape
    columns = raw.shape[0]
    tile = min(TILE, columns)
    whole = lambda a: pl.BlockSpec(a.shape, lambda j: (0, 0), pipeline_mode=pl.Buffered(1))
    tall = pl.BlockSpec((tile, rank), lambda j: (j, 0))
    return pl.pallas_call(
        update_kernel,
        grid=(columns // tile,),
        in_specs=[whole(q_hi), whole(q_lo), whole(inv_norm), tall],
        out_specs=[pl.BlockSpec((rows, tile), lambda j: (0, j)), tall],
        out_shape=[
            jax.ShapeDtypeStruct((rows, columns), BF16),
            jax.ShapeDtypeStruct((columns, rank), F32),
        ],
        compiler_params=pltpu.CompilerParams(
            dimension_semantics=("arbitrary",), vmem_limit_bytes=40 << 20
        ),
        cost_estimate=pl.CostEstimate(
            flops=6 * rows * columns * rank,
            transcendentals=0,
            bytes_accessed=columns * (2 * rows + 8 * rank),
        ),
        name="update",
    )(q_hi, q_lo, inv_norm, raw)


def eliminate(block, unroll):
    size = block.shape[0]
    rows = lax.broadcasted_iota(jnp.int32, (size, size), 0)
    lanes = lax.broadcasted_iota(jnp.int32, (size, size), 1)
    row = lax.broadcasted_iota(jnp.int32, (size, 1), 0)

    def lane(j, work):
        return jnp.sum(jnp.where(lanes == j, work, 0.0), axis=1, keepdims=True)

    def entry(j, column):
        return jnp.sum(jnp.where(row == j, column, 0.0), axis=0, keepdims=True)

    def step(j, carry):
        work, inverse, pivots, column = carry
        here = rows == j
        ahead = lane(j + 1, work)
        across = jnp.sum(jnp.where(here, work, 0.0), axis=0, keepdims=True)
        beside = jnp.sum(jnp.where(here, inverse, 0.0), axis=0, keepdims=True)
        pivot = entry(j, column)
        factor = jnp.where(row > j, column / pivot, 0.0)
        work = work - factor * across
        inverse = inverse - factor * beside
        ahead = ahead - factor * entry(j + 1, column)
        return work, inverse, jnp.where(row == j, pivot, pivots), ahead

    start = (block, (rows == lanes).astype(F32), jnp.ones((size, 1), F32), lane(0, block))
    _, inverse, pivots, _ = lax.fori_loop(0, size, step, start, unroll=unroll)
    return inverse * (1.0 / jnp.sqrt(pivots))


def inverse_kernel(first, size, *refs):
    work_in, inverse_in = refs[0], refs[-3]
    work, inverse = refs[-2:]
    total = work.shape[0]
    last = first + size
    work[...] = work_in[...]
    if first:
        inverse[...] = inverse_in[...]
    else:
        rows = lax.broadcasted_iota(jnp.int32, (total, total), 0)
        lanes = lax.broadcasted_iota(jnp.int32, (total, total), 1)
        inverse[...] = (rows == lanes).astype(F32)
    block = eliminate(work[first:last, first:last], UNROLL)
    strip = dot(block, inverse[first:last, :], 1, 0, HIGHEST)
    inverse[first:last, :] = strip
    if last < total:
        panel = dot(work[last:, first:last], block, 1, 1, HIGHEST)
        inverse[last:, :] = inverse[last:, :] - dot(panel, strip, 1, 0, HIGHEST)
        work[last:, last:] = work[last:, last:] - dot(panel, panel, 1, 1, HIGHEST)


def cholesky_inverse(gram):
    total = gram.shape[0]
    size = min(BLOCK, total)
    state = [gram]
    for first in range(0, total, size):
        state = pl.pallas_call(
            lambda *refs, first=first: inverse_kernel(first, size, *refs),
            out_shape=[jax.ShapeDtypeStruct(gram.shape, F32)] * 2,
            compiler_params=pltpu.CompilerParams(vmem_limit_bytes=24 << 20),
            name="cholesky_inverse",
        )(*state)
    return state[1]


def body(outer, dout, din, activations, grad_out, momentum, right_factor):
    wide = Ring("wide", outer, lax.axis_size("wide") // outer)
    narrow = Ring("narrow", lax.axis_size("narrow") // CORES, CORES)
    rank = right_factor.shape[1]
    tokens, columns = activations.shape
    members, seats = wide.outer * wide.inner, narrow.outer * narrow.inner
    halves = 2 if columns % (2 * members * LANES) == 0 else 1
    width = columns // halves
    strip = width // members
    quarter = rank // seats

    v_hi, v_lo = split(right_factor)
    av = dot(activations, v_hi, 1, 0) + dot(activations, v_lo, 1, 0)
    av = narrow_sum(narrow, av, quarter)
    av_hi, av_lo = split(wide.blocks(av))

    acts = [
        wide.gather(activations[:, h * width : (h + 1) * width], spread=wide.inner == 2)
        for h in range(halves)
    ]
    all_grads = narrow_collect(narrow, grad_out, 0)
    grads = jnp.concatenate(
        [
            lax.dynamic_slice_in_dim(all_grads, wide.at(-s, -d) * tokens, tokens, 0)
            for s, d in wide.order()
        ],
        axis=0,
    ).T

    mv = dot(momentum, right_factor, 1, 0, HIGH)
    mv = narrow_sum(narrow, mv, quarter)
    left_part = mv + (dot(grads, av_hi, 1, 0) + dot(grads, av_lo, 1, 0))
    left = narrow_collect(narrow, left_part, 1)

    gram_part = dot(left_part, left, 0, 0, HIGHEST)
    gram = narrow_collect(narrow, wide.total(gram_part), 0)
    inverse = cholesky_inverse(gram)
    ortho = dot(left, inverse, 1, 1, HIGH)

    left_hi, left_lo = split(left.T)
    buffer, shares = None, []
    for h in range(halves):
        buffer, product = buffer_call(h, grads, left_hi, left_lo, momentum, acts[h], buffer)
        shares.append(
            wide.scatter_sum(
                lambda index, p=product: lax.dynamic_slice_in_dim(p, index * strip, strip, 1),
            )
        )

    share = dot(jnp.concatenate(shares, axis=1), inverse, 0, 1, HIGHEST)
    own = jnp.sum(share * share, axis=0)
    size = jnp.sqrt(own / share.shape[0])
    exponent = jnp.floor(jnp.log2(jnp.where(size > 0, size, 1.0)))
    sent = jnp.concatenate(
        [
            (share * jnp.exp2(-exponent)[None, :]).astype(F16),
            jnp.broadcast_to(exponent.astype(F16)[None, :], (PAD, rank)),
        ],
        axis=0,
    )
    feedback_left = (FEEDBACK * ortho).astype(BF16)
    gathered = dict(zip(wide.order(), wide.gather(sent, spread=wide.inner == 2)))
    pieces, starts, squares = [], [], []
    for s in range(wide.outer):
        rights, places = [], []
        for d in range(wide.inner):
            got = gathered[s, d]
            value = got[:-PAD].astype(F32) * jnp.exp2(got[-PAD : -PAD + 1].astype(F32))
            value = lax.optimization_barrier(value)
            for h in range(halves):
                place = h * members + wide.at(-s, -d)
                rights.append(value[h * strip : (h + 1) * strip])
                places.append(place)
                starts.append(place * strip)
        pieces += rights
        buffer, square = feedback_call(feedback_left, buffer, rights, jnp.stack(places))
        squares.append(square)
    raw = put(pieces, starts, (columns, rank), 0)
    col_squares = narrow.total(sum(squares))
    inv_norm = 1.0 / (jnp.sqrt(col_squares) + EPSILON)
    q_hi, q_lo = split(ortho * (math.sqrt(dout * din / rank) * inv_norm))
    update, new_right = update_call(q_hi, q_lo, inv_norm, raw)
    return buffer, new_right, update


def solution(mesh):
    members = mesh.shape["wide"]
    outer = 1 << -(-(members.bit_length() - 1) // 2)

    def local(dout, din, *arrays):
        return body(outer, dout, din, *arrays)

    def whole(activations, grad_out, momentum, right_factor):
        dout, din = momentum.shape
        return jax.shard_map(
            lambda *arrays: local(dout, din, *arrays),
            mesh=mesh,
            in_specs=(P("wide", "narrow"), P("narrow", "wide"), P("wide", "narrow"), P("narrow", None)),
            out_specs=(P("wide", "narrow"), P("narrow", None), P("wide", "narrow")),
            check_vma=False,
        )(activations, grad_out, momentum, right_factor)

    return whole
```

```python
import math

import jax
import jax.numpy as jnp
from jax import lax
from jax.experimental import pallas as pl
from jax.experimental.pallas import tpu as pltpu
from jax.sharding import PartitionSpec as P


FEEDBACK = 0.05
EPSILON = 1e-06
LANES = 128
CORES = 2
TILE = 512
PAD = 16
BLOCK = 128
UNROLL = 8

HIGH = lax.Precision.HIGH
HIGHEST = lax.Precision.HIGHEST
F32 = jnp.float32
F16 = jnp.float16
BF16 = jnp.bfloat16


def split(x):
    hi = lax.reduce_precision(x, exponent_bits=8, mantissa_bits=7)
    return hi.astype(BF16), (x - hi).astype(BF16)


def dot(a, b, ca, cb, precision=None):
    return lax.dot_general(
        a, b, (((ca,), (cb,)), ((), ())), precision=precision, preferred_element_type=F32
    )


def put(pieces, starts, shape, axis):
    out = jnp.zeros(shape, pieces[0].dtype)
    for piece, start in zip(pieces, starts):
        out = lax.dynamic_update_slice_in_dim(out, piece, start, axis)
    return out


class Ring:
    def __init__(self, name, outer, inner):
        self.name, self.outer, self.inner = name, outer, inner
        index = lax.axis_index(name)
        self.o, self.i = index // inner, lax.rem(index, inner)

    def send(self, x, do, di):
        o, i = self.outer, self.inner
        if do % o == 0 and di % i == 0:
            return x
        pairs = [
            (a * i + b, ((a + do) % o) * i + (b + di) % i) for a in range(o) for b in range(i)
        ]
        return lax.ppermute(x, self.name, pairs)

    def at(self, do, di):
        o, i = self.outer, self.inner
        return lax.rem(self.o + do % o, o) * i + lax.rem(self.i + di % i, i)

    def order(self):
        return [(s, d) for s in range(self.outer) for d in range(self.inner)]

    def blocks(self, x):
        found = []
        for s, d in self.order():
            found.append(self.send(x, s, d))
        return jnp.concatenate(found, axis=0)

    def gather(self, x, spread=False):
        found, held, aside = {}, x, {}
        for s in range(self.outer):
            held = self.send(held, 1, 0) if s else held
            found[s, 0] = held
            for d in range(1, self.inner):
                if spread and s == self.outer - 1:
                    half = x.shape[1] // 2
                    near = self.send(held[:, :half], 0, d)
                    far = self.send(aside[d][:, half:], 1, 0)
                    found[s, d] = jnp.concatenate([near, far], axis=1)
                else:
                    aside[d] = found[s, d] = self.send(held, 0, d)
        return [found[key] for key in self.order()]

    def scatter_sum(self, piece):
        total = None
        for j in range(self.outer):
            back = -1 - j
            mine = piece(self.at(back, 0))
            for d in range(1, self.inner):
                got = self.send(piece(self.at(back, d)), 0, d)
                mine = mine + got
            if total is not None:
                total = self.send(total, 1, 0)
            total = mine if total is None else total + mine
        return total

    def total(self, x):
        count, step = self.outer * self.inner, 1
        while step < count:
            got = lax.ppermute(x, self.name, [(k, k ^ step) for k in range(count)])
            x = x + got
            step *= 2
        return x


def narrow_sum(ring, x, width):
    cut = lambda index: lax.dynamic_slice_in_dim(x, index * width, width, 1)
    keep = [cut(ring.at(s, 0)) for s in range(ring.outer)]
    give = [cut(ring.at(s, 1)) for s in range(ring.outer)]
    got = ring.send(jnp.concatenate(give, axis=1), 0, 1)
    kept = [k + got[:, s * width : (s + 1) * width] for s, k in enumerate(keep)]
    total = kept[0]
    for s in range(1, ring.outer):
        got = ring.send(kept[s], s, 0)
        total = total + got
    return total


def narrow_collect(ring, x, axis):
    size = x.shape[axis]
    shape = list(x.shape)
    shape[axis] = size * ring.outer * ring.inner
    mine = []
    for s in range(ring.outer):
        mine.append(ring.send(x, s, 0))
    other = ring.send(jnp.concatenate(mine, axis=axis), 0, 1)
    pieces, starts = [], []
    for s in range(ring.outer):
        pieces += [mine[s], lax.slice_in_dim(other, s * size, (s + 1) * size, axis=axis)]
        starts += [ring.at(-s, 0) * size, ring.at(-s, 1) * size]
    return put(pieces, starts, shape, axis)


def buffer_kernel(count, grads, left_hi, left_lo, momentum, *refs):
    acts, (buffer_out, product_out) = refs[:count], refs[-2:]
    rows = jnp.concatenate([a[...] for a in acts], axis=0)
    buffer = momentum[...] + jnp.dot(grads[...], rows, preferred_element_type=F32)
    buffer_out[...] = buffer
    hi = buffer.astype(BF16)
    lo = (buffer - hi.astype(F32)).astype(BF16)
    product = jnp.dot(left_hi[...], hi, preferred_element_type=F32)
    product += jnp.dot(left_hi[...], lo, preferred_element_type=F32)
    product += jnp.dot(left_lo[...], hi, preferred_element_type=F32)
    product_out[...] = product


def buffer_call(half, grads, left_hi, left_lo, momentum, acts, buffer):
    rows, columns = momentum.shape
    rank = left_hi.shape[0]
    width = acts[0].shape[1]
    tile = min(TILE, width)
    first = half * width // tile
    resident = lambda a: pl.BlockSpec(a.shape, lambda j: (0, 0), pipeline_mode=pl.Buffered(1))
    moving = lambda r: pl.BlockSpec((r, tile), lambda j: (0, j))
    placed = pl.BlockSpec((rows, tile), lambda j: (0, first + j))
    in_specs = [resident(grads), resident(left_hi), resident(left_lo), placed]
    in_specs += [moving(a.shape[0]) for a in acts]
    args = [grads, left_hi, left_lo, momentum, *acts]
    aliases = {}
    if buffer is not None:
        aliases = {len(args): 0}
        in_specs.append(pl.BlockSpec(memory_space=pl.ANY))
        args.append(buffer)
    tokens = grads.shape[1]
    flops = 2 * rows * width * (tokens + 3 * rank)
    count = len(acts)
    return pl.pallas_call(
        lambda *refs: buffer_kernel(count, *refs),
        grid=(width // tile,),
        in_specs=in_specs,
        out_specs=[placed, moving(rank)],
        out_shape=[
            jax.ShapeDtypeStruct((rows, columns), F32),
            jax.ShapeDtypeStruct((rank, width), F32),
        ],
        input_output_aliases=aliases,
        compiler_params=pltpu.CompilerParams(
            dimension_semantics=("arbitrary",), vmem_limit_bytes=56 << 20
        ),
        cost_estimate=pl.CostEstimate(
            flops=flops, transcendentals=0, bytes_accessed=width * (8 * rows + 2 * tokens + 4 * rank)
        ),
        name="buffer_product",
    )(*args)


def output_kernel(places, ortho, q_hi, q_lo, inv_norm, buffer, right, *refs):
    del places
    momentum, normalized, update = refs[-3:]
    value = right[...]
    hi = value.astype(BF16)
    lo = (value - hi.astype(F32)).astype(BF16)
    momentum[...] = buffer[...] - dot(ortho[...], hi, 1, 1)
    normalized[...] = value * inv_norm[...]
    product = dot(q_hi[...], hi, 1, 1) + dot(q_hi[...], lo, 1, 1) + dot(q_lo[...], hi, 1, 1)
    update[...] = product.astype(BF16)


def output_call(ortho, q_hi, q_lo, inv_norm, outs, right, places, strip):
    rows, columns = outs[0].shape
    rank = right.shape[1]
    count = right.shape[0] // strip
    whole = lambda a: pl.BlockSpec(a.shape, lambda k, p: (0, 0), pipeline_mode=pl.Buffered(1))
    placed = pl.BlockSpec((rows, strip), lambda k, p: (0, p[k]))
    fixed = [ortho, q_hi, q_lo, inv_norm]
    args = [places, *fixed, outs[0], right, *outs[1:]]
    in_specs = [whole(a) for a in fixed] + [placed]
    in_specs += [pl.BlockSpec((strip, rank), lambda k, p: (k, 0))]
    in_specs += [pl.BlockSpec(memory_space=pl.ANY) for _ in outs[1:]]
    aliases = {5: 0}
    aliases.update({7 + k: 1 + k for k in range(len(outs) - 1)})
    return pl.pallas_call(
        output_kernel,
        grid_spec=pltpu.PrefetchScalarGridSpec(
            num_scalar_prefetch=1,
            grid=(count,),
            in_specs=in_specs,
            out_specs=[placed, pl.BlockSpec((strip, rank), lambda k, p: (p[k], 0)), placed],
        ),
        out_shape=[
            jax.ShapeDtypeStruct((rows, columns), F32),
            jax.ShapeDtypeStruct((columns, rank), F32),
            jax.ShapeDtypeStruct((rows, columns), BF16),
        ],
        input_output_aliases=aliases,
        compiler_params=pltpu.CompilerParams(
            dimension_semantics=("arbitrary",), vmem_limit_bytes=32 << 20
        ),
        cost_estimate=pl.CostEstimate(
            flops=8 * rows * strip * rank * count,
            transcendentals=0,
            bytes_accessed=10 * rows * strip * count,
        ),
        name="outputs",
    )(*args)


def eliminate(block, unroll):
    size = block.shape[0]
    rows = lax.broadcasted_iota(jnp.int32, (size, size), 0)
    lanes = lax.broadcasted_iota(jnp.int32, (size, size), 1)
    row = lax.broadcasted_iota(jnp.int32, (size, 1), 0)

    def lane(j, work):
        return jnp.sum(jnp.where(lanes == j, work, 0.0), axis=1, keepdims=True)

    def entry(j, column):
        return jnp.sum(jnp.where(row == j, column, 0.0), axis=0, keepdims=True)

    def step(j, carry):
        work, inverse, pivots, column = carry
        here = rows == j
        ahead = lane(j + 1, work)
        across = jnp.sum(jnp.where(here, work, 0.0), axis=0, keepdims=True)
        beside = jnp.sum(jnp.where(here, inverse, 0.0), axis=0, keepdims=True)
        pivot = entry(j, column)
        factor = jnp.where(row > j, column / pivot, 0.0)
        work = work - factor * across
        inverse = inverse - factor * beside
        ahead = ahead - factor * entry(j + 1, column)
        return work, inverse, jnp.where(row == j, pivot, pivots), ahead

    start = (block, (rows == lanes).astype(F32), jnp.ones((size, 1), F32), lane(0, block))
    _, inverse, pivots, _ = lax.fori_loop(0, size, step, start, unroll=unroll)
    return inverse * (1.0 / jnp.sqrt(pivots))


def inverse_kernel(first, size, *refs):
    work_in, inverse_in = refs[0], refs[-3]
    work, inverse = refs[-2:]
    total = work.shape[0]
    last = first + size
    work[...] = work_in[...]
    if first:
        inverse[...] = inverse_in[...]
    else:
        rows = lax.broadcasted_iota(jnp.int32, (total, total), 0)
        lanes = lax.broadcasted_iota(jnp.int32, (total, total), 1)
        inverse[...] = (rows == lanes).astype(F32)
    block = eliminate(work[first:last, first:last], UNROLL)
    strip = dot(block, inverse[first:last, :], 1, 0, HIGHEST)
    inverse[first:last, :] = strip
    if last < total:
        panel = dot(work[last:, first:last], block, 1, 1, HIGHEST)
        inverse[last:, :] = inverse[last:, :] - dot(panel, strip, 1, 0, HIGHEST)
        work[last:, last:] = work[last:, last:] - dot(panel, panel, 1, 1, HIGHEST)


def cholesky_inverse(gram):
    total = gram.shape[0]
    size = min(BLOCK, total)
    state = [gram]
    for first in range(0, total, size):
        state = pl.pallas_call(
            lambda *refs, first=first: inverse_kernel(first, size, *refs),
            out_shape=[jax.ShapeDtypeStruct(gram.shape, F32)] * 2,
            compiler_params=pltpu.CompilerParams(vmem_limit_bytes=24 << 20),
            name="cholesky_inverse",
        )(*state)
    return state[1]


def body(outer, dout, din, activations, grad_out, momentum, right_factor):
    wide = Ring("wide", outer, lax.axis_size("wide") // outer)
    narrow = Ring("narrow", lax.axis_size("narrow") // CORES, CORES)
    rank = right_factor.shape[1]
    tokens, columns = activations.shape
    members, seats = wide.outer * wide.inner, narrow.outer * narrow.inner
    halves = 2 if columns % (2 * members * LANES) == 0 else 1
    width = columns // halves
    strip = width // members
    quarter = rank // seats

    v_hi, v_lo = split(right_factor)
    av = dot(activations, v_hi, 1, 0) + dot(activations, v_lo, 1, 0)
    av = narrow_sum(narrow, av, quarter)
    av_hi, av_lo = split(wide.blocks(av))

    acts = [
        wide.gather(activations[:, h * width : (h + 1) * width], spread=wide.inner == 2)
        for h in range(halves)
    ]
    all_grads = narrow_collect(narrow, grad_out, 0)
    grads = jnp.concatenate(
        [
            lax.dynamic_slice_in_dim(all_grads, wide.at(-s, -d) * tokens, tokens, 0)
            for s, d in wide.order()
        ],
        axis=0,
    ).T

    mv = dot(momentum, right_factor, 1, 0, HIGH)
    mv = narrow_sum(narrow, mv, quarter)
    left_part = mv + (dot(grads, av_hi, 1, 0) + dot(grads, av_lo, 1, 0))
    left = narrow_collect(narrow, left_part, 1)

    gram_part = dot(left_part, left, 0, 0, HIGHEST)
    gram = narrow_collect(narrow, wide.total(gram_part), 0)
    inverse = cholesky_inverse(gram)
    ortho = dot(left, inverse, 1, 1, HIGH)

    left_hi, left_lo = split(left.T)
    buffer, shares = None, []
    for h in range(halves):
        buffer, product = buffer_call(h, grads, left_hi, left_lo, momentum, acts[h], buffer)
        shares.append(
            wide.scatter_sum(
                lambda index, p=product: lax.dynamic_slice_in_dim(p, index * strip, strip, 1),
            )
        )

    share = dot(jnp.concatenate(shares, axis=1), inverse, 0, 1, HIGHEST)
    own = jnp.sum(share * share, axis=0)
    size = jnp.sqrt(own / share.shape[0])
    exponent = jnp.floor(jnp.log2(jnp.where(size > 0, size, 1.0)))
    sent = jnp.concatenate(
        [
            (share * jnp.exp2(-exponent)[None, :]).astype(F16),
            jnp.broadcast_to(exponent.astype(F16)[None, :], (PAD, rank)),
        ],
        axis=0,
    )
    col_squares = wide.total(narrow.total(own[None, :]))
    feedback_left = (FEEDBACK * ortho).astype(BF16)
    gathered = dict(zip(wide.order(), wide.gather(sent, spread=wide.inner == 2)))
    inv_norm = 1.0 / (jnp.sqrt(col_squares) + EPSILON)
    q_hi, q_lo = split(ortho * (math.sqrt(dout * din / rank) * inv_norm))
    outs = [buffer]
    for s in range(wide.outer):
        rights, places = [], []
        for d in range(wide.inner):
            got = gathered[s, d]
            rights.append(got[:-PAD].astype(F32) * jnp.exp2(got[-PAD : -PAD + 1].astype(F32)))
            places += [h * members + wide.at(-s, -d) for h in range(halves)]
        right = lax.optimization_barrier(jnp.concatenate(rights, axis=0))
        outs = output_call(
            feedback_left, q_hi, q_lo, inv_norm, outs, right, jnp.stack(places), strip
        )
    return tuple(outs)


def solution(mesh):
    members = mesh.shape["wide"]
    outer = 1 << -(-(members.bit_length() - 1) // 2)

    def local(dout, din, *arrays):
        return body(outer, dout, din, *arrays)

    def whole(activations, grad_out, momentum, right_factor):
        dout, din = momentum.shape
        return jax.shard_map(
            lambda *arrays: local(dout, din, *arrays),
            mesh=mesh,
            in_specs=(P("wide", "narrow"), P("narrow", "wide"), P("wide", "narrow"), P("narrow", None)),
            out_specs=(P("wide", "narrow"), P("narrow", None), P("wide", "narrow")),
            check_vma=False,
        )(activations, grad_out, momentum, right_factor)

    return whole
```
